32 devices in a mesh: grp: 8 (over z, x), sub: 4 (over y, core).
Axes of the slice: x: 2, y: 2, z: 4, core: 2. Of those that a mesh axis runs over, the one named last changes fastest.
Arguments:
- gate_source: bfloat16 [32, 2048, 768], P('grp', 'sub'), may hold values from -0.125 to 0.125
- up_source: bfloat16 [32, 2048, 768], P('grp', 'sub'), may hold values from -0.125 to 0.125
- down_source: bfloat16 [32, 2048, 768], P('grp', 'sub'), may hold values from -0.21875 to 0.21875
- source_order: int32 [32], replicated, may hold values from 0 to 31, each once
- target_order: int32 [32], replicated, may hold values from 0 to 31, each once
Outputs:
- packed: bfloat16 [3, 8, 4, 8, 96, 2048], P(None, 'grp', 'sub')
- scales: float32 [3, 8, 4, 16, 768], P(None, 'grp', 'sub')
The draws below stay inside these ranges and needn't reach their ends.
Inputs may be any that keep to these rules, and one draw needn't show every extreme that they name: `source_order`: each expert number appears once. `target_order`: each expert number appears once.
All inputs are finite; a program needn't handle non-finite values. Where the reference program divides by a largest or mean magnitude, that divisor is 1e-20 or more.
Results may differ from the reference program's by a relative error of at most 0.001.
Values may be sent and summed in bfloat16 or wider, within the bound.
A program may use at most 192 MiB of HBM per device.

```python
import jax
import jax.numpy as jnp
from jax import lax

D = 2048
FF = 768
BLOCK = 128
E = 32
EPT = 8
FFT = 96
N_GRP = 8
N_SUB = 4


def levels(rng, shape, shards, smallest, largest):
    def one(position, blocks):
        steps = jax.random.uniform(jax.random.fold_in(jax.random.fold_in(rng, 6), position), (blocks,), jnp.float32, smallest / len(shards), largest / len(shards))
        return jnp.repeat(jnp.exp(steps), shape[position] // blocks).reshape((-1,) + (1,) * (len(shape) - position - 1))

    level = one(*shards[0])
    for cut in shards[1:]:
        level = level * one(*cut)
    return level


def bell_draw(own_key, shape, spread, most, cuts=(), kind=jnp.bfloat16):
    entries = spread * jax.random.normal(own_key, shape, jnp.float32)
    if cuts:
        entries = entries * levels(own_key, shape, cuts, -0.22, 0.18)
    return jnp.clip(entries, -most, most).astype(kind)


def setup_inputs(seed: int = 0) -> dict:
    splits = jax.random.split(jax.random.key(seed), 6)
    return {
        "gate_source": bell_draw(splits[0], (E, D, FF), D ** -0.5, 0.125, ((0, 8), (1, 4))),
        "up_source": bell_draw(splits[1], (E, D, FF), D ** -0.5, 0.125, ((0, 8), (1, 4))),
        "down_source": bell_draw(splits[2], (E, D, FF), FF ** -0.5, 0.21875, ((0, 8), (1, 4))),
        "source_order": jax.random.permutation(splits[3], E).astype(jnp.int32),
        "target_order": jax.random.permutation(splits[4], E).astype(jnp.int32),
    }


EPS = 1e-6


def pack_layout(quantized):
    values = quantized.reshape(N_GRP // 2, EPT, D, 2, N_SUB, FFT)
    values = values.transpose(0, 3, 4, 1, 5, 2)
    return values.reshape(N_GRP, N_SUB, EPT, FFT, D)


def scale_layout(block_scale):
    values = block_scale.reshape(N_GRP // 2, EPT, D // BLOCK, 2, N_SUB, FFT)
    values = values.transpose(0, 3, 4, 2, 1, 5)
    return values.reshape(N_GRP, N_SUB, D // BLOCK, EPT * FFT)


def convert(weights, picked):
    def convert_one(target):
        matrix = weights[picked[target]].astype(jnp.float32).reshape(D // BLOCK, BLOCK, FF)
        block_scale = jnp.max(jnp.abs(matrix), axis=1) + EPS
        quantized = (matrix / block_scale[:, None, :]).astype(jnp.bfloat16).reshape(D, FF)
        return quantized, block_scale

    quantized, block_scale = lax.map(convert_one, jnp.arange(E, dtype=jnp.int32))
    return pack_layout(quantized), scale_layout(block_scale)


def reference(gate_source, up_source, down_source, source_order, target_order):
    matches = (source_order[None, :] == target_order[:, None]).astype(jnp.int32)
    picked = jnp.sum(matches * jnp.arange(E, dtype=jnp.int32)[None, :], axis=1).astype(jnp.int32)
    gate_q, gate_s = convert(gate_source, picked)
    up_q, up_s = convert(up_source, picked)
    down_q, down_s = convert(down_source, picked)
    return jnp.stack([gate_q, up_q, down_q]), jnp.stack([gate_s, up_s, down_s])
```

```python
import functools

import jax
import jax.numpy as jnp
from jax import lax
from jax.experimental import pallas as pl
from jax.experimental.pallas import tpu as pltpu
from jax.sharding import PartitionSpec as P

BLOCK = 128
EPS = 1e-06
MESH = pl.DeviceIdType.MESH
PIECES = 3
CAPS = (8, 9, 10, 12)


def pick(source_order, target_order):
    matches = source_order[None, :] == target_order[:, None]
    slots = jnp.arange(source_order.shape[0], dtype=jnp.int32)
    return jnp.sum(jnp.where(matches, slots[None, :], 0), axis=1, dtype=jnp.int32)


def plain(gate_source, up_source, down_source, source_order, target_order):
    stacked = jnp.stack([gate_source, up_source, down_source])
    matrices, local_slots, local_rows, hidden = stacked.shape
    groups = lax.axis_size("grp")
    shards = lax.axis_size("sub")
    devices = groups * shards
    experts = local_slots * groups
    full_rows = local_rows * shards
    targets = groups // 2
    per_group = experts // targets
    splits = 2 * shards
    columns = hidden // splits
    picked = pick(source_order, target_order)
    slab_rows = local_rows // devices
    pieces = stacked.reshape(matrices, 1, local_slots, devices, slab_rows, hidden)
    received = lax.all_to_all(pieces, ("grp", "sub"), split_axis=3, concat_axis=1, tiled=True)
    received = received.reshape(matrices, groups, shards, local_slots, slab_rows, hidden)
    received = received.transpose(0, 1, 3, 2, 4, 5).reshape(
        matrices, experts, shards * slab_rows, hidden
    )
    ordered = jnp.take(received, picked, axis=1)
    outgoing = ordered.reshape(matrices, targets, per_group, shards * slab_rows, splits, columns)
    outgoing = outgoing.transpose(0, 1, 4, 2, 3, 5).reshape(
        matrices, devices, per_group, 1, shards * slab_rows, columns
    )
    placed = lax.all_to_all(outgoing, ("grp", "sub"), split_axis=1, concat_axis=3, tiled=True)
    placed = placed.reshape(matrices, per_group, devices, shards, slab_rows, columns)
    placed = placed.transpose(0, 1, 3, 2, 4, 5).reshape(matrices, per_group, full_rows, columns)
    num_blocks = full_rows // BLOCK
    blocks = placed.astype(jnp.float32).reshape(matrices, per_group, num_blocks, BLOCK, columns)
    block_scale = jnp.max(jnp.abs(blocks), axis=3) + EPS
    quantized = (blocks / block_scale[:, :, :, None, :]).astype(jnp.bfloat16)
    quantized = quantized.reshape(matrices, per_group, full_rows, columns).transpose(0, 1, 3, 2)
    quantized = quantized.reshape(matrices, 1, 1, per_group, columns, full_rows)
    block_scale = block_scale.transpose(0, 2, 1, 3).reshape(
        matrices, 1, 1, num_blocks, per_group * columns
    )
    return (quantized, block_scale)


def routes(source_order, target_order, per_zone):
    experts = source_order.shape[0]
    zone = lax.axis_index("grp") // 2
    slots = jnp.arange(experts, dtype=jnp.int32)
    matches = source_order[:, None] == target_order[None, :]
    goes = jnp.sum(jnp.where(matches, slots[None, :], 0), axis=1, dtype=jnp.int32)
    here, there = slots // per_zone, goes // per_zone

    def outer(z):
        return (z == 0) | (z == 3)

    def rank(chosen, key):
        before = chosen[None, :] & (key[None, :] == key[:, None]) & (slots[None, :] < slots[:, None])
        return jnp.sum(before.astype(jnp.int32), axis=1)

    leaves = outer(here) & (there != here)
    crosses = (here // 2) != (there // 2)
    enters = outer(there) & (there != here)
    rank_in, rank_mid, rank_out = rank(leaves, here), rank(crosses, here // 2), rank(enters, there)
    own = slots % per_zone
    on_inner = jnp.where(outer(here), per_zone + rank_in, own)
    after_mid = jnp.where(crosses, 2 * per_zone + rank_mid, on_inner)
    last = jnp.where(here == there, own, jnp.where(outer(there), per_zone + rank_out, after_mid))

    def listed(chosen, position, value, length):
        hit = chosen[None, :] & (position[None, :] == jnp.arange(length, dtype=jnp.int32)[:, None])
        return jnp.sum(jnp.where(hit, value[None, :], 0), axis=1, dtype=jnp.int32)

    inward = listed(leaves & (here == zone), rank_in, own, per_zone)
    outward = listed(enters & (there // 2 == zone // 2), rank_out, after_mid, per_zone)
    beside = jnp.where(outer(zone), inward, outward)
    middle = listed(crosses & (here // 2 == zone // 2), rank_mid, on_inner, 2 * per_zone)
    keep = listed(there == zone, goes % per_zone, last, per_zone)
    load = jnp.sum((crosses & (here < 2)).astype(jnp.int32))
    return jnp.concatenate([beside, middle, keep]), load


def line_kernel(cap, per_zone, shards, columns, *refs):
    table, sources, packed, scales = refs[0], refs[1:4], refs[4], refs[5]
    steps = len(sources) * PIECES
    scratch = refs[6:]
    held, crossed, beside, middle, out = (
        scratch[0:steps],
        scratch[steps : 2 * steps],
        scratch[2 * steps : 3 * steps],
        scratch[3 * steps : 4 * steps],
        scratch[4 * steps : 4 * steps + 2],
    )
    sems = scratch[4 * steps + 2 :]
    ex_send, ex_recv, ex_own, be_send, be_recv, mi_send, mi_recv, out_sem = sems
    grp, sub = lax.axis_index("grp"), lax.axis_index("sub")
    zone, half = grp // 2, grp % 2
    splits = 2 * shards
    me = half * shards + sub
    local = sources[0].shape[0]
    rows = sources[0].shape[2]
    piece = columns // PIECES
    blocks = rows * shards // BLOCK
    is_outer = (zone == 0) | (zone == 3)
    is_inner = (zone == 1) | (zone == 2)
    neighbour = (zone + 1 - 2 * (zone % 2)) * 2 + half
    across = (3 - zone) * 2 + half

    def place(j, who):
        return held[j].at[
            pl.ds((who // shards) * local, local),
            :,
            pl.ds(pl.multiple_of((who % shards) * rows, BLOCK), rows),
        ]

    def part(j, who):
        start = pl.multiple_of(who * columns + (j % PIECES) * piece, 16)
        return sources[j // PIECES].at[:, pl.ds(start, piece), :]

    def exchange(j, d):
        to = lax.rem(me + d, splits)
        return pltpu.make_async_remote_copy(
            src_ref=part(j, to), dst_ref=place(j, me), send_sem=ex_send.at[j, d], recv_sem=ex_recv.at[j, d],
            device_id=((zone * 2 + to // shards), to % shards), device_id_type=MESH,
        )

    def keep_own(j):
        return pltpu.make_async_copy(part(j, me), place(j, me), ex_own.at[j])

    def send_beside(j):
        return pltpu.make_async_remote_copy(
            src_ref=beside[j], dst_ref=held[j].at[pl.ds(per_zone, per_zone)], send_sem=be_send.at[j],
            recv_sem=be_recv.at[j], device_id=(neighbour, sub), device_id_type=MESH,
        )

    def send_middle(j):
        return pltpu.make_async_remote_copy(
            src_ref=middle[j], dst_ref=crossed[j], send_sem=mi_send.at[j],
            recv_sem=mi_recv.at[j], device_id=(across, sub), device_id_type=MESH,
        )

    def write_out(j):
        f0 = (j % PIECES) * piece
        return pltpu.make_async_copy(
            out[j % 2], packed.at[j // PIECES, :, pl.ds(f0, piece), :], out_sem.at[j % 2]
        )

    def start_exchange(j):
        for d in range(1, splits):
            exchange(j, d).start()
        keep_own(j).start()

    def wait_exchange(j):
        for d in range(1, splits):
            exchange(j, d).wait_recv()
        keep_own(j).wait()

    def from_held(j, i):
        return held[j][i]

    def from_either(j, i):
        a = held[j][jnp.minimum(i, 2 * per_zone - 1)]
        b = crossed[j][jnp.maximum(i - 2 * per_zone, 0)]
        return jnp.where(i < 2 * per_zone, a, b)

    def finish(j, read):
        f0 = (j % PIECES) * piece
        if j >= 2:
            write_out(j - 2).wait()

        def one(k, _):
            x = read(j, table[3 * per_zone + k]).astype(jnp.float32)
            lanes = lax.broadcasted_iota(jnp.int32, (piece, BLOCK), 1)
            kept = jnp.zeros((piece, BLOCK), jnp.float32)
            for b in range(blocks):
                xb = x[:, b * BLOCK : (b + 1) * BLOCK]
                scale = jnp.max(jnp.abs(xb), axis=1, keepdims=True) + EPS
                out[j % 2][k, :, b * BLOCK : (b + 1) * BLOCK] = (xb * (1.0 / scale)).astype(jnp.bfloat16)
                kept = jnp.where(lanes == b, scale, kept)
            scales[j // PIECES, k, f0 : f0 + piece, :] = kept
            return 0

        lax.fori_loop(0, per_zone, one, 0)
        write_out(j).start()

    ahead = 2
    for j in range(ahead):
        start_exchange(j)
    for t in range(steps + 3):
        if t + ahead < steps:
            start_exchange(t + ahead)

        @pl.when(is_outer)
        def _():
            if t < steps:
                wait_exchange(t)

                def put(k, _):
                    beside[t][k] = from_held(t, table[k])
                    return 0

                lax.fori_loop(0, per_zone, put, 0)
                send_beside(t).start()
            if t >= 3:
                send_beside(t - 3).wait_recv()
                finish(t - 3, from_held)

        @pl.when(is_inner)
        def _():
            j = t - 1
            if 0 <= j < steps:
                wait_exchange(j)
                send_beside(j).wait_recv()

                def put(k, _):
                    middle[j][k] = from_held(j, table[per_zone + k])
                    return 0

                lax.fori_loop(0, cap, put, 0)
                send_middle(j).start()
            i = t - 2
            if 0 <= i < steps:
                send_middle(i).wait_recv()

                def put2(k, _):
                    beside[i][k] = from_either(i, table[k])
                    return 0

                lax.fori_loop(0, per_zone, put2, 0)
                send_beside(i).start()
                finish(i, from_either)

    for j in range(steps):
        for d in range(1, splits):
            exchange(j, d).wait_send()
        send_beside(j).wait_send()

    @pl.when(is_inner)
    def _():
        for j in range(steps):
            send_middle(j).wait_send()

    for j in range(max(steps - 2, 0), steps):
        write_out(j).wait()


def line(cap, per_zone, shards, table, sources):
    local, hidden, rows = sources[0].shape
    columns = hidden // (2 * shards)
    piece = columns // PIECES
    steps = len(sources) * PIECES
    full = rows * shards
    bf16 = jnp.bfloat16
    scratch = (
        [pltpu.VMEM((2 * per_zone, piece, full), bf16)] * steps
        + [pltpu.VMEM((cap, piece, full), bf16)] * steps
        + [pltpu.VMEM((per_zone, piece, full), bf16)] * steps
        + [pltpu.VMEM((cap, piece, full), bf16)] * steps
        + [pltpu.VMEM((per_zone, piece, full), bf16)] * 2
        + [
            pltpu.SemaphoreType.DMA((steps, 2 * shards)),
            pltpu.SemaphoreType.DMA((steps, 2 * shards)),
            pltpu.SemaphoreType.DMA((steps,)),
            pltpu.SemaphoreType.DMA((steps,)),
            pltpu.SemaphoreType.DMA((steps,)),
            pltpu.SemaphoreType.DMA((steps,)),
            pltpu.SemaphoreType.DMA((steps,)),
            pltpu.SemaphoreType.DMA((2,)),
        ]
    )
    packed, scales = pl.pallas_call(
        functools.partial(line_kernel, cap, per_zone, shards, columns),
        out_shape=(
            jax.ShapeDtypeStruct((len(sources), per_zone, columns, full), bf16),
            jax.ShapeDtypeStruct((len(sources), per_zone, columns, BLOCK), jnp.float32),
        ),
        in_specs=[pl.BlockSpec(memory_space=pltpu.SMEM)] + [pl.BlockSpec(memory_space=pl.ANY)] * len(sources),
        out_specs=(pl.BlockSpec(memory_space=pl.ANY), pl.BlockSpec(memory_space=pltpu.VMEM)),
        scratch_shapes=scratch,
        compiler_params=pltpu.CompilerParams(has_side_effects=True, vmem_limit_bytes=67043328),
        name=f"line_{cap}",
    )(table, *sources)
    blocks = full // BLOCK
    scales = scales[..., :blocks].transpose(0, 3, 1, 2)
    return (
        packed.reshape(len(sources), 1, 1, per_zone, columns, full),
        scales.reshape(len(sources), 1, 1, blocks, per_zone * columns),
    )


def per_device(gate_source, up_source, down_source, source_order, target_order):
    groups, shards = lax.axis_size("grp"), lax.axis_size("sub")
    given = (gate_source, up_source, down_source, source_order, target_order)
    if groups != 8:
        return plain(*given)
    per_zone = 2 * gate_source.shape[0]
    table, load = routes(source_order, target_order, per_zone)

    def routed(cap):
        def run(given, table):
            sources = [w.transpose(0, 2, 1) for w in given[:3]]
            return line(cap, per_zone, shards, table, sources)

        return run

    index = jnp.sum((load > jnp.array(CAPS, jnp.int32)).astype(jnp.int32))
    branches = [routed(cap) for cap in CAPS] + [lambda given, table: plain(*given)]
    return lax.switch(index, branches, given, table)


def solution(mesh):
    placed = (P("grp", "sub", None), P("grp", "sub", None), P("grp", "sub", None), P(), P())
    return jax.shard_map(
        per_device,
        mesh=mesh,
        in_specs=placed,
        out_specs=(P(None, "grp", "sub", None, None, None), P(None, "grp", "sub", None, None)),
        check_vma=False,
    )
```

```python
import functools

import jax
import jax.numpy as jnp
from jax import lax
from jax.experimental import pallas as pl
from jax.experimental.pallas import tpu as pltpu
from jax.sharding import PartitionSpec as P

BLOCK = 128
EPS = 1e-06
MESH = pl.DeviceIdType.MESH
PIECES = 6
CAPS = (7, 8, 9, 11)


def pick(source_order, target_order):
    matches = source_order[None, :] == target_order[:, None]
    slots = jnp.arange(source_order.shape[0], dtype=jnp.int32)
    return jnp.sum(jnp.where(matches, slots[None, :], 0), axis=1, dtype=jnp.int32)


def plain(gate_source, up_source, down_source, source_order, target_order):
    stacked = jnp.stack([gate_source, up_source, down_source])
    matrices, local_slots, local_rows, hidden = stacked.shape
    groups = lax.axis_size("grp")
    shards = lax.axis_size("sub")
    devices = groups * shards
    experts = local_slots * groups
    full_rows = local_rows * shards
    targets = groups // 2
    per_group = experts // targets
    splits = 2 * shards
    columns = hidden // splits
    picked = pick(source_order, target_order)
    slab_rows = local_rows // devices
    pieces = stacked.reshape(matrices, 1, local_slots, devices, slab_rows, hidden)
    received = lax.all_to_all(pieces, ("grp", "sub"), split_axis=3, concat_axis=1, tiled=True)
    received = received.reshape(matrices, groups, shards, local_slots, slab_rows, hidden)
    received = received.transpose(0, 1, 3, 2, 4, 5).reshape(
        matrices, experts, shards * slab_rows, hidden
    )
    ordered = jnp.take(received, picked, axis=1)
    outgoing = ordered.reshape(matrices, targets, per_group, shards * slab_rows, splits, columns)
    outgoing = outgoing.transpose(0, 1, 4, 2, 3, 5).reshape(
        matrices, devices, per_group, 1, shards * slab_rows, columns
    )
    placed = lax.all_to_all(outgoing, ("grp", "sub"), split_axis=1, concat_axis=3, tiled=True)
    placed = placed.reshape(matrices, per_group, devices, shards, slab_rows, columns)
    placed = placed.transpose(0, 1, 3, 2, 4, 5).reshape(matrices, per_group, full_rows, columns)
    num_blocks = full_rows // BLOCK
    blocks = placed.astype(jnp.float32).reshape(matrices, per_group, num_blocks, BLOCK, columns)
    block_scale = jnp.max(jnp.abs(blocks), axis=3) + EPS
    quantized = (blocks / block_scale[:, :, :, None, :]).astype(jnp.bfloat16)
    quantized = quantized.reshape(matrices, per_group, full_rows, columns).transpose(0, 1, 3, 2)
    quantized = quantized.reshape(matrices, 1, 1, per_group, columns, full_rows)
    block_scale = block_scale.transpose(0, 2, 1, 3).reshape(
        matrices, 1, 1, num_blocks, per_group * columns
    )
    return (quantized, block_scale)


def routes(source_order, target_order, per_zone):
    experts = source_order.shape[0]
    zone = lax.axis_index("grp") // 2
    slots = jnp.arange(experts, dtype=jnp.int32)
    matches = source_order[:, None] == target_order[None, :]
    goes = jnp.sum(jnp.where(matches, slots[None, :], 0), axis=1, dtype=jnp.int32)
    here, there = slots // per_zone, goes // per_zone

    def outer(z):
        return (z == 0) | (z == 3)

    def rank(chosen, key):
        before = chosen[None, :] & (key[None, :] == key[:, None]) & (slots[None, :] < slots[:, None])
        return jnp.sum(before.astype(jnp.int32), axis=1)

    leaves = outer(here) & (there != here)
    crosses = (here // 2) != (there // 2)
    enters = outer(there) & (there != here)
    rank_in, rank_mid, rank_out = rank(leaves, here), rank(crosses, here // 2), rank(enters, there)
    own = slots % per_zone
    on_inner = jnp.where(outer(here), per_zone + rank_in, own)
    after_mid = jnp.where(crosses, 2 * per_zone + rank_mid, on_inner)
    last = jnp.where(here == there, own, jnp.where(outer(there), per_zone + rank_out, after_mid))

    def listed(chosen, position, value, length):
        hit = chosen[None, :] & (position[None, :] == jnp.arange(length, dtype=jnp.int32)[:, None])
        return jnp.sum(jnp.where(hit, value[None, :], 0), axis=1, dtype=jnp.int32)

    inward = listed(leaves & (here == zone), rank_in, own, per_zone)
    outward = listed(enters & (there // 2 == zone // 2), rank_out, after_mid, per_zone)
    beside = jnp.where(outer(zone), inward, outward)
    middle = listed(crosses & (here // 2 == zone // 2), rank_mid, on_inner, 2 * per_zone)
    keep = listed(there == zone, goes % per_zone, last, per_zone)
    counts = [crosses & (here < 2), leaves & (here == 0), leaves & (here == 3)]
    load = jnp.max(jnp.stack([jnp.sum(c.astype(jnp.int32)) for c in counts]))
    return jnp.concatenate([beside, middle, keep]), load


def line_kernel(cap, per_zone, shards, columns, *refs):
    table, sources, packed, scales = refs[0], refs[1:4], refs[4], refs[5]
    steps = len(sources) * PIECES
    scratch = refs[6:]
    held, crossed, beside, middle, out = (
        scratch[0:steps],
        scratch[steps : 2 * steps],
        scratch[2 * steps : 3 * steps],
        scratch[3 * steps : 4 * steps],
        scratch[4 * steps : 4 * steps + 2],
    )
    sems = scratch[4 * steps + 2 :]
    ex_send, ex_recv, ex_own, be_send, be_recv, mi_send, mi_recv, out_sem = sems
    grp, sub = lax.axis_index("grp"), lax.axis_index("sub")
    zone, half = grp // 2, grp % 2
    splits = 2 * shards
    me = half * shards + sub
    local = sources[0].shape[0]
    rows = sources[0].shape[2]
    piece = columns // PIECES
    edge = min(cap, per_zone)
    blocks = rows * shards // BLOCK
    is_outer = (zone == 0) | (zone == 3)
    is_inner = (zone == 1) | (zone == 2)
    neighbour = (zone + 1 - 2 * (zone % 2)) * 2 + half
    across = (3 - zone) * 2 + half

    def place(j, who):
        return held[j].at[
            pl.ds((who // shards) * local, local),
            :,
            pl.ds(pl.multiple_of((who % shards) * rows, BLOCK), rows),
        ]

    def part(j, who):
        start = pl.multiple_of(who * columns + (j % PIECES) * piece, 16)
        return sources[j // PIECES].at[:, pl.ds(start, piece), :]

    def exchange(j, d):
        to = lax.rem(me + d, splits)
        return pltpu.make_async_remote_copy(
            src_ref=part(j, to), dst_ref=place(j, me), send_sem=ex_send.at[j, d], recv_sem=ex_recv.at[j, d],
            device_id=((zone * 2 + to // shards), to % shards), device_id_type=MESH,
        )

    def keep_own(j):
        return pltpu.make_async_copy(part(j, me), place(j, me), ex_own.at[j])

    def send_beside(j):
        return pltpu.make_async_remote_copy(
            src_ref=beside[j], dst_ref=held[j].at[pl.ds(per_zone, edge)], send_sem=be_send.at[j],
            recv_sem=be_recv.at[j], device_id=(neighbour, sub), device_id_type=MESH,
        )

    def send_middle(j):
        return pltpu.make_async_remote_copy(
            src_ref=middle[j], dst_ref=crossed[j], send_sem=mi_send.at[j],
            recv_sem=mi_recv.at[j], device_id=(across, sub), device_id_type=MESH,
        )

    def write_out(j):
        f0 = (j % PIECES) * piece
        return pltpu.make_async_copy(
            out[j % 2], packed.at[j // PIECES, :, pl.ds(f0, piece), :], out_sem.at[j % 2]
        )

    def start_exchange(j):
        def go(d, _):
            exchange(j, d).start()
            return 0

        lax.fori_loop(1, splits, go, 0)
        keep_own(j).start()

    def wait_exchange(j):
        def arrive(d, _):
            exchange(j, d).wait_recv()
            return 0

        lax.fori_loop(1, splits, arrive, 0)
        keep_own(j).wait()

    def from_held(j, i):
        return held[j][i]

    def from_either(j, i):
        a = held[j][jnp.minimum(i, 2 * per_zone - 1)]
        b = crossed[j][jnp.maximum(i - 2 * per_zone, 0)]
        return jnp.where(i < 2 * per_zone, a, b)

    def finish(j, read):
        f0 = (j % PIECES) * piece
        if j >= 2:
            write_out(j - 2).wait()

        def one(k, _):
            x = read(j, table[3 * per_zone + k]).astype(jnp.float32)
            lanes = lax.broadcasted_iota(jnp.int32, (piece, BLOCK), 1)
            kept = jnp.zeros((piece, BLOCK), jnp.float32)
            for b in range(blocks):
                xb = x[:, b * BLOCK : (b + 1) * BLOCK]
                scale = jnp.max(jnp.abs(xb), axis=1, keepdims=True) + EPS
                out[j % 2][k, :, b * BLOCK : (b + 1) * BLOCK] = (xb * (1.0 / scale)).astype(jnp.bfloat16)
                kept = jnp.where(lanes == b, scale, kept)
            scales[j // PIECES, k, f0 : f0 + piece, :] = kept
            return 0

        lax.fori_loop(0, per_zone, one, 0)
        write_out(j).start()

    ahead, lag = 2, 4
    for j in range(ahead):
        start_exchange(j)
    for t in range(steps + lag):
        if t + ahead < steps:
            start_exchange(t + ahead)

        @pl.when(is_outer)
        def _():
            if t < steps:
                wait_exchange(t)

                def put(k, _):
                    beside[t][k] = from_held(t, table[k])
                    return 0

                lax.fori_loop(0, edge, put, 0)
                send_beside(t).start()
            if t >= lag:
                send_beside(t - lag).wait_recv()

        @pl.when(is_inner)
        def _():
            j = t - 1
            if 0 <= j < steps:
                wait_exchange(j)
                send_beside(j).wait_recv()

                def put(k, _):
                    middle[j][k] = from_held(j, table[per_zone + k])
                    return 0

                lax.fori_loop(0, cap, put, 0)
                send_middle(j).start()
            i = t - 2
            if 0 <= i < steps:
                send_middle(i).wait_recv()

                def put2(k, _):
                    beside[i][k] = from_either(i, table[k])
                    return 0

                lax.fori_loop(0, edge, put2, 0)
                send_beside(i).start()

        if t >= lag:
            finish(t - lag, from_either)

    for j in range(steps):
        def gone(d, _):
            exchange(j, d).wait_send()
            return 0

        lax.fori_loop(1, splits, gone, 0)
        send_beside(j).wait_send()

    @pl.when(is_inner)
    def _():
        for j in range(steps):
            send_middle(j).wait_send()

    for j in range(max(steps - 2, 0), steps):
        write_out(j).wait()


def line(cap, per_zone, shards, table, sources):
    local, hidden, rows = sources[0].shape
    columns = hidden // (2 * shards)
    piece = columns // PIECES
    steps = len(sources) * PIECES
    full = rows * shards
    bf16 = jnp.bfloat16
    scratch = (
        [pltpu.VMEM((2 * per_zone, piece, full), bf16)] * steps
        + [pltpu.VMEM((cap, piece, full), bf16)] * steps
        + [pltpu.VMEM((min(cap, per_zone), piece, full), bf16)] * steps
        + [pltpu.VMEM((cap, piece, full), bf16)] * steps
        + [pltpu.VMEM((per_zone, piece, full), bf16)] * 2
        + [
            pltpu.SemaphoreType.DMA((steps, 2 * shards)),
            pltpu.SemaphoreType.DMA((steps, 2 * shards)),
            pltpu.SemaphoreType.DMA((steps,)),
            pltpu.SemaphoreType.DMA((steps,)),
            pltpu.SemaphoreType.DMA((steps,)),
            pltpu.SemaphoreType.DMA((steps,)),
            pltpu.SemaphoreType.DMA((steps,)),
            pltpu.SemaphoreType.DMA((2,)),
        ]
    )
    packed, scales = pl.pallas_call(
        functools.partial(line_kernel, cap, per_zone, shards, columns),
        out_shape=(
            jax.ShapeDtypeStruct((len(sources), per_zone, columns, full), bf16),
            jax.ShapeDtypeStruct((len(sources), per_zone, columns, BLOCK), jnp.float32),
        ),
        in_specs=[pl.BlockSpec(memory_space=pltpu.SMEM)] + [pl.BlockSpec(memory_space=pl.ANY)] * len(sources),
        out_specs=(pl.BlockSpec(memory_space=pl.ANY), pl.BlockSpec(memory_space=pltpu.VMEM)),
        scratch_shapes=scratch,
        compiler_params=pltpu.CompilerParams(has_side_effects=True, vmem_limit_bytes=67043328),
        name=f"line_{cap}",
    )(table, *sources)
    blocks = full // BLOCK
    scales = scales[..., :blocks].transpose(0, 3, 1, 2)
    return (
        packed.reshape(len(sources), 1, 1, per_zone, columns, full),
        scales.reshape(len(sources), 1, 1, blocks, per_zone * columns),
    )


def per_device(gate_source, up_source, down_source, source_order, target_order):
    groups, shards = lax.axis_size("grp"), lax.axis_size("sub")
    given = (gate_source, up_source, down_source, source_order, target_order)
    if groups != 8:
        return plain(*given)
    per_zone = 2 * gate_source.shape[0]
    table, load = routes(source_order, target_order, per_zone)

    def routed(cap):
        def run(given, table):
            sources = [w.transpose(0, 2, 1) for w in given[:3]]
            return line(cap, per_zone, shards, table, sources)

        return run

    index = jnp.sum((load > jnp.array(CAPS, jnp.int32)).astype(jnp.int32))
    branches = [routed(cap) for cap in CAPS] + [lambda given, table: plain(*given)]
    return lax.switch(index, branches, given, table)


def solution(mesh):
    placed = (P("grp", "sub", None), P("grp", "sub", None), P("grp", "sub", None), P(), P())
    return jax.shard_map(
        per_device,
        mesh=mesh,
        in_specs=placed,
        out_specs=(P(None, "grp", "sub", None, None, None), P(None, "grp", "sub", None, None)),
        check_vma=False,
    )
```
